32 devices in a mesh: groups: 2 (over y), seq: 4 (over z), head: 2 (over x), sub: 2 (over core).
Axes of the slice: x: 2, y: 2, z: 4, core: 2. Of those that a mesh axis runs over, the one named last changes fastest.
Arguments:
- queries: bfloat16 [8192, 4096], P(('groups', 'seq'), 'head'), parts along dimension 0, may hold values from -48 to 48
- keys: bfloat16 [8192, 1024], P(('groups', 'seq', 'sub'), 'head'), parts along dimension 0, may hold values from -18 to 18
- values: bfloat16 [8192, 1024], P(('groups', 'seq', 'sub'), 'head'), parts along dimension 0, may hold values from -6 to 6
- doc_lengths: int32 [16], P('groups'), parts along dimension 0, may hold values from 1 to 2048, 4096 in all
Outputs:
- attended: bfloat16 [8192, 4096], P(('groups', 'seq'), 'head'), parts along dimension 0
The draws below stay inside these ranges and needn't reach their ends.
There are 2 independent parts, one for each index of `groups`. The reference program is written for one: setup_inputs(seed, part) draws one part's arguments, and reference() takes and returns one part's arrays. A program takes and returns all parts, laid end to end along the dimension named above; each array names one. Nothing has to cross between parts.
Inputs may be any that keep to these rules, and one draw needn't show every extreme that they name: `doc_lengths`: the 8 lengths sum to 4096; one of them is exactly 2048.
All inputs are finite; a program needn't handle non-finite values.
Results may differ from the reference program's by a relative error of at most 0.0036.
Values may be sent and summed in bfloat16 or wider, within the bound.
A program may use at most 192 MiB of HBM per device.

```python
import math
import jax
import jax.numpy as jnp
import numpy as np
from jax import lax

QH = 32
KVH = 8
DH = 128
TOK_DEV = 1024
SEQLEN = 4096
NDOCS = 8
MAXDOC = 2048
N_SEQ = 4


def shared_rows(key):
    width = KVH * DH
    drawn = jnp.clip(jax.random.normal(jax.random.fold_in(key, 11), (SEQLEN, width), jnp.float32), -6.0, 6.0)
    return drawn


def draw_keys(key, part):
    drawn = shared_rows(key)
    return drawn.astype(jnp.bfloat16)


def draw_queries(key, part):
    base_rows = jnp.clip(jax.random.normal(jax.random.fold_in(key, 19), (SEQLEN, QH * DH), jnp.float32), -6.0, 6.0)
    return base_rows.astype(jnp.bfloat16)


def levels(rng, extent, pieces, low, high):
    gain = 1.0
    for axis_at, parts in pieces:
        heights = jax.random.uniform(jax.random.fold_in(jax.random.fold_in(rng, 6), axis_at), (parts,), jnp.float32, low / len(pieces), high / len(pieces))
        gain = gain * jnp.repeat(jnp.exp(heights), extent[axis_at] // parts).reshape((-1,) + (1,) * (len(extent) - 1 - axis_at))
    return gain


def profile(number_of, total, reach, skew):
    loads = [(1 << 20) // math.isqrt(rank ** skew) + 1 for rank in range(2, number_of + 1)]
    spare, counts = total - reach - (number_of - 1), [1] * (number_of - 1)
    while spare > 0:
        candidates = [i for i in range(number_of - 1) if counts[i] < reach]
        mass, budget = sum([loads[i] for i in candidates]), spare
        for i in candidates:
            more = min(reach - counts[i], max(1, budget * loads[i] // mass), spare)
            counts[i] = counts[i] + more
            spare = spare - more
    return np.array([reach] + counts)


def ragged(key, number_of, total, reach, slope):
    if number_of == 2:
        one = jax.random.randint(key, (), max(1, total - reach), min(reach, total - 1) + 1)
        return jnp.stack([one, total - one])
    tallies = jnp.asarray(profile(number_of, total, reach, slope), jnp.int32)
    couples = (number_of - 1) // 2
    source_of, taker = tallies[1:1 + 2 * couples:2], tallies[2:2 + 2 * couples:2]
    margin = jnp.minimum(source_of - 1, reach - taker)
    moved = jax.random.randint(jax.random.fold_in(key, 1), (couples,), 0, 1 << 20) % (margin + 1)
    tallies = tallies.at[1:1 + 2 * couples:2].set(source_of - moved).at[2:2 + 2 * couples:2].set(taker + moved)
    return tallies[jax.random.permutation(jax.random.fold_in(key, 2), number_of)]


def centred(own_key, extent, scale, bound, split=(), held_as=jnp.bfloat16):
    level = levels(own_key, extent, split, -0.22, 0.18) if split else 1.0
    array = jax.random.normal(own_key, extent, jnp.float32) * scale * level
    return jnp.minimum(jnp.maximum(array, -bound), bound).astype(held_as)


def setup_inputs(seed: int = 0, part: int = 0) -> dict:
    key_of = jax.random.split(jax.random.key(seed), 5)
    part_keys = jax.random.split(jax.random.fold_in(key_of[4], part), 5)
    queries = draw_queries(jax.random.fold_in(jax.random.fold_in(key_of[4], part), 71), part)
    keys = draw_keys(jax.random.fold_in(jax.random.fold_in(key_of[4], part), 71), part)
    values = centred(part_keys[2], (SEQLEN, KVH * DH), 1.0, 6.0, ((0, 8), (1, 2)))
    doc_lengths = ragged(part_keys[3], NDOCS, SEQLEN, MAXDOC, 2).astype(jnp.int32)
    return {"queries": queries, "keys": keys, "values": values, "doc_lengths": doc_lengths}


def reference(queries, keys, values, doc_lengths):
    per_group = QH // KVH
    window = MAXDOC + TOK_DEV
    starts = jnp.cumsum(doc_lengths) - doc_lengths
    positions = jnp.arange(SEQLEN, dtype=jnp.int32)
    doc_of = lax.optimization_barrier(jnp.sum((starts[None, :] <= positions[:, None]).astype(jnp.int32), axis=1)) - 1
    padded_keys = jnp.concatenate([jnp.zeros((MAXDOC, KVH * DH), keys.dtype), keys], axis=0)
    padded_values = jnp.concatenate([jnp.zeros((MAXDOC, KVH * DH), values.dtype), values], axis=0)
    padded_docs = jnp.concatenate([jnp.full((MAXDOC,), -1, jnp.int32), doc_of.astype(jnp.int32)], axis=0)
    scaling = 1.0 / math.sqrt(DH)

    def one_block(number):
        first = (number * TOK_DEV).astype(jnp.int32)
        query_rows = lax.dynamic_slice_in_dim(queries, first, TOK_DEV, 0).astype(jnp.float32)
        query_rows = query_rows.reshape(TOK_DEV, KVH, per_group, DH)
        key_rows = lax.dynamic_slice_in_dim(padded_keys, first, window, 0).astype(jnp.float32)
        value_rows = lax.dynamic_slice_in_dim(padded_values, first, window, 0).astype(jnp.float32)
        query_pos = first + jnp.arange(TOK_DEV, dtype=jnp.int32)
        query_doc = lax.dynamic_slice_in_dim(doc_of.astype(jnp.int32), first, TOK_DEV, 0)
        key_pos = first - MAXDOC + jnp.arange(window, dtype=jnp.int32)
        key_doc = lax.dynamic_slice_in_dim(padded_docs, first, window, 0)
        allowed = (key_pos[None, :] <= query_pos[:, None]) & (key_doc[None, :] == query_doc[:, None])
        outputs = []
        for head_pair in range(KVH):
            head_keys = key_rows[:, head_pair * DH:(head_pair + 1) * DH]
            head_values = value_rows[:, head_pair * DH:(head_pair + 1) * DH]
            scores = jnp.einsum('qgd,kd->qgk', query_rows[:, head_pair], head_keys) * scaling
            scores = jnp.where(allowed[:, None, :], scores, -jnp.inf)
            highest = lax.optimization_barrier(jnp.max(scores, axis=-1))
            expo = jnp.exp(scores - highest[..., None])
            denom = lax.optimization_barrier(jnp.sum(expo, axis=-1))
            weight = lax.optimization_barrier(expo.astype(jnp.bfloat16)).astype(jnp.float32)
            summed = jnp.einsum('qgk,kd->qgd', weight, head_values)
            outputs.append(summed / denom[..., None])
        stacked = jnp.stack(outputs, axis=1)
        return stacked.reshape(TOK_DEV, QH * DH).astype(jnp.bfloat16)
    result = lax.map(one_block, jnp.arange(N_SEQ, dtype=jnp.int32))
    return result.reshape(SEQLEN, QH * DH)
```

```python
import functools
import math

import jax
import jax.numpy as jnp
from jax import lax
from jax.experimental import pallas as pl
from jax.experimental.pallas import tpu as pltpu
from jax.sharding import PartitionSpec as P

DH = 128
SPAN = 2
LANES = 128
BLOCKED = -1048576.0
LEAST = -1e30
MESH = pl.DeviceIdType.MESH
SCALE = math.log2(math.e) / math.sqrt(DH)


def attention_kernel(
    sizes, lengths, q_hbm, k_hbm, v_hbm, out,
    q_vm, kbuf, vbuf, qx, kx, top, acc, obuf,
    load_sem, swap_sem, hop_sem, recv_sem, out_send, out_recv, out_local,
):
    n_seq, rows, half, kv_cols, q_cols, split_kv, n_docs, rows_q = sizes
    seq, sub = lax.axis_index("seq"), lax.axis_index("sub")
    other = 1 - sub
    heads, kv_heads = q_cols // DH, kv_cols // DH
    group = heads // kv_heads
    has_prev, has_next = seq > 0, seq < n_seq - 1

    my_cols = pl.ds(pl.multiple_of(sub * kv_cols, LANES), kv_cols) if split_kv else pl.ds(0, kv_cols)
    its_cols = pl.ds(pl.multiple_of(other * kv_cols, LANES), kv_cols) if split_kv else pl.ds(0, kv_cols)
    my_q = pl.ds(pl.multiple_of(sub * q_cols, LANES), q_cols)

    loads = [
        pltpu.make_async_copy(k_hbm.at[:, my_cols], kbuf.at[0, sub], load_sem.at[0]),
        pltpu.make_async_copy(v_hbm.at[:, my_cols], vbuf.at[0, sub], load_sem.at[1]),
        pltpu.make_async_copy(q_hbm.at[:, my_q], q_vm, load_sem.at[2]),
    ]
    for load in loads:
        load.start()

    barrier = pltpu.get_barrier_semaphore()
    pl.semaphore_signal(barrier, inc=1, device_id={"sub": other}, device_id_type=MESH)

    @pl.when(has_prev)
    def _():
        pl.semaphore_signal(barrier, inc=1, device_id={"seq": seq - 1}, device_id_type=MESH)

    @pl.when(has_next)
    def _():
        pl.semaphore_signal(barrier, inc=1, device_id={"seq": seq + 1}, device_id_type=MESH)

    peers = 1 + jnp.minimum(seq, 1) + jnp.minimum(n_seq - 1 - seq, 1)
    pl.semaphore_wait(barrier, peers)

    def remote(src, dst, send, recv, where):
        return pltpu.make_async_remote_copy(
            src_ref=src, dst_ref=dst, send_sem=send, recv_sem=recv, device_id=where, device_id_type=MESH
        )

    swaps = [
        remote(hbm.at[:, its_cols], buf.at[0, sub], swap_sem.at[kind], recv_sem.at[0, sub, kind], {"sub": other})
        for kind, (hbm, buf) in enumerate(((k_hbm, kbuf), (v_hbm, vbuf)))
    ]
    for swap in swaps:
        swap.start()

    def hops(slot, part):
        return [
            remote(
                buf.at[slot, part], buf.at[slot + 1, part],
                hop_sem.at[slot, part, kind], recv_sem.at[slot + 1, part, kind], {"seq": seq + 1},
            )
            for kind, buf in enumerate((kbuf, vbuf))
        ]

    def wait_arrival(slot, part):
        for kind, buf in enumerate((kbuf, vbuf)):
            pltpu.make_async_copy(buf.at[slot, part], buf.at[slot, part], recv_sem.at[slot, part, kind]).wait()

    def start_hops(slot, part):
        @pl.when(has_next)
        def _():
            for hop in hops(slot, part):
                hop.start()

    loads[0].wait()
    loads[1].wait()
    start_hops(0, sub)

    lane = lax.broadcasted_iota(jnp.int32, (1, LANES), 1)
    lows = jnp.full((1, LANES), 2**30, jnp.int32)
    highs = jnp.full((1, LANES), 2**30, jnp.int32)
    begin = jnp.int32(0)
    for d in range(n_docs):
        end = begin + lengths[d]
        lows = jnp.where(lane == d, begin, lows)
        highs = jnp.where(lane == d, end, highs)
        begin = end
    block = 256

    def fill(i, _):
        row0 = pl.multiple_of(i * block, block)
        base = lax.broadcasted_iota(jnp.int32, (block, LANES), 0) + row0 + seq * rows
        for slot in range(SPAN + 1):
            place = base - slot * rows
            inside = (place >= lows) & (place < highs)
            kx[slot, pl.ds(row0, block), :] = jnp.where(inside, 1.0, 0.0).astype(jnp.bfloat16)
            if slot == 0:
                qx[pl.ds(row0, block), :] = jnp.where(inside, 0.0, BLOCKED).astype(jnp.bfloat16)
        return 0

    lax.fori_loop(0, rows // block, fill, 0)

    wait_arrival(0, other)
    start_hops(0, other)
    loads[2].wait()

    ones = jnp.ones((half, DH), jnp.bfloat16)

    def wide(x, times):
        return jnp.concatenate([x] * times, axis=1)

    def update(slot, part, row0, kv, first, offset):
        keys = jnp.concatenate(
            [kbuf[slot, part, :, pl.ds(pl.multiple_of(kv * DH, DH), DH)],
             kx[slot, pl.ds(pl.multiple_of(part * half, half), half), :]], axis=1)
        vals = jnp.concatenate([vbuf[slot, part, :, pl.ds(pl.multiple_of(kv * DH, DH), DH)], ones], axis=1)
        q_rows = pl.ds(row0, rows_q)
        if offset is not None:
            row_at = lax.broadcasted_iota(jnp.int32, (rows_q, half), 0) + offset
            causal = lax.broadcasted_iota(jnp.int32, (rows_q, half), 1) <= row_at
        for g in range(group):
            h = kv * group + g
            query = jnp.concatenate(
                [q_vm[q_rows, pl.ds(pl.multiple_of(h * DH, DH), DH)], qx[q_rows, :]], axis=1)
            scores = lax.dot_general(
                query, keys, (((1,), (1,)), ((), ())), preferred_element_type=jnp.float32)
            if offset is not None:
                scores = jnp.where(causal, scores, LEAST)
            peak = jnp.max(scores, axis=1, keepdims=True)
            if first:
                new_top = jnp.broadcast_to(peak, (rows_q, LANES))
            else:
                old_top = top[h, q_rows, :]
                new_top = jnp.maximum(old_top, peak)
            weights = jnp.exp2((scores - wide(new_top, half // LANES)) * SCALE).astype(jnp.bfloat16)
            product = jnp.dot(weights, vals, preferred_element_type=jnp.float32)
            if first:
                acc[h, q_rows, :] = product
            else:
                factor = jnp.exp2((old_top - new_top) * SCALE)
                acc[h, q_rows, :] = acc[h, q_rows, :] * wide(factor, 2) + product
            top[h, q_rows, :] = new_top

    per_half = half // rows_q

    def sweep(slot, part, start, count, first, diagonal):
        def body(i, _):
            block_at, kv = i // kv_heads, i % kv_heads
            row0 = pl.multiple_of(start + block_at * rows_q, rows_q)
            update(slot, part, row0, kv, first, block_at * rows_q if diagonal else None)
            return 0

        lax.fori_loop(0, count * kv_heads, body, 0)

    sweep(0, 0, 0, per_half, True, True)
    sweep(0, 1, half, per_half, True, True)
    sweep(0, 0, half, per_half, False, False)

    for slot in range(1, SPAN + 1):
        @pl.when(seq >= slot)
        def _():
            for part in (sub, other):
                wait_arrival(slot, part)
                if slot < SPAN:
                    start_hops(slot, part)
                sweep(slot, part, 0, rows // rows_q, False, False)

    def sends(h):
        columns = pl.ds(pl.multiple_of(sub * q_cols + h * DH, DH), DH)
        return (
            remote(obuf.at[h], out.at[:, columns], out_send.at[h], out_recv.at[h], {"sub": other}),
            pltpu.make_async_copy(obuf.at[h], out.at[:, columns], out_local.at[h]),
        )

    for h in range(heads):
        obuf[h] = (acc[h, :, :DH] / acc[h, :, DH:]).astype(jnp.bfloat16)
        if h:
            for copy in sends(h - 1):
                copy.start()
    for h in range(heads):
        far, near = sends(h)
        if h == 0:
            near.wait()
            for copy in sends(heads - 1):
                copy.start()
        else:
            near.wait()
        far.wait()

    for swap in swaps:
        swap.wait_send()

    @pl.when(has_next)
    def _():
        for part in (sub, other):
            for hop in hops(0, part):
                hop.wait_send()

    for slot in range(1, SPAN):
        @pl.when((seq >= slot) & has_next)
        def _():
            for part in (sub, other):
                for hop in hops(slot, part):
                    hop.wait_send()


def shards(n_seq, queries, keys, values, doc_lengths):
    rows, q_total = queries.shape
    half, kv_total = keys.shape
    q_cols = q_total // 2
    split_kv = kv_total // DH >= 2
    kv_cols = kv_total // 2 if split_kv else kv_total
    heads = q_cols // DH
    sizes = (n_seq, rows, half, kv_cols, q_cols, split_kv, doc_lengths.shape[0], min(256, half))
    any_space = pl.BlockSpec(memory_space=pl.ANY)
    dma = pltpu.SemaphoreType.DMA
    return pl.pallas_call(
        functools.partial(attention_kernel, sizes),
        out_shape=jax.ShapeDtypeStruct((rows, q_total), jnp.bfloat16),
        in_specs=[pl.BlockSpec(memory_space=pltpu.SMEM)] + [any_space] * 3,
        out_specs=any_space,
        scratch_shapes=[
            pltpu.VMEM((rows, q_cols), jnp.bfloat16),
            pltpu.VMEM((SPAN + 1, 2, half, kv_cols), jnp.bfloat16),
            pltpu.VMEM((SPAN + 1, 2, half, kv_cols), jnp.bfloat16),
            pltpu.VMEM((rows, LANES), jnp.bfloat16),
            pltpu.VMEM((SPAN + 1, rows, LANES), jnp.bfloat16),
            pltpu.VMEM((heads, rows, LANES), jnp.float32),
            pltpu.VMEM((heads, rows, 2 * DH), jnp.float32),
            pltpu.VMEM((heads, rows, DH), jnp.bfloat16),
            dma((3,)),
            dma((2,)),
            dma((SPAN, 2, 2)),
            dma((SPAN + 1, 2, 2)),
            dma((heads,)),
            dma((heads,)),
            dma((heads,)),
        ],
        compiler_params=pltpu.CompilerParams(
            collective_id=0, has_side_effects=True, vmem_limit_bytes=60 * 1024 * 1024
        ),
    )(doc_lengths, queries, keys, values)


def solution(mesh):
    placed = (
        P(("groups", "seq"), "head"),
        P(("groups", "seq", "sub"), "head"),
        P(("groups", "seq", "sub"), "head"),
        P("groups"),
    )
    return jax.shard_map(
        functools.partial(shards, mesh.shape["seq"]),
        mesh=mesh, in_specs=placed, out_specs=P(("groups", "seq"), "head"), check_vma=False,
    )
```

```python
import functools
import math

import jax
import jax.numpy as jnp
from jax import lax
from jax.experimental import pallas as pl
from jax.experimental.pallas import tpu as pltpu
from jax.sharding import PartitionSpec as P

DH = 128
SPAN = 2
LANES = 128
BLOCKED = -1048576.0
LEAST = -1e30
MESH = pl.DeviceIdType.MESH
SCALE = math.log2(math.e) / math.sqrt(DH)


def attention_kernel(
    sizes, lengths, q_hbm, k_hbm, v_hbm, out,
    q_vm, kbuf, vbuf, qx, kx, top, acc, obuf,
    load_sem, swap_sem, hop_sem, recv_sem, out_send, out_recv, out_local,
):
    n_seq, rows, half, kv_cols, q_cols, split_kv, n_docs, rows_q, pieces = sizes
    piece_rows = half // pieces
    seq, sub = lax.axis_index("seq"), lax.axis_index("sub")
    other = 1 - sub
    heads, kv_heads = q_cols // DH, kv_cols // DH
    group = heads // kv_heads
    has_prev, has_next = seq > 0, seq < n_seq - 1

    my_cols = pl.ds(pl.multiple_of(sub * kv_cols, LANES), kv_cols) if split_kv else pl.ds(0, kv_cols)
    its_cols = pl.ds(pl.multiple_of(other * kv_cols, LANES), kv_cols) if split_kv else pl.ds(0, kv_cols)
    my_q = pl.ds(pl.multiple_of(sub * q_cols, LANES), q_cols)

    loads = [
        pltpu.make_async_copy(k_hbm.at[:, my_cols], kbuf.at[0, sub], load_sem.at[0]),
        pltpu.make_async_copy(v_hbm.at[:, my_cols], vbuf.at[0, sub], load_sem.at[1]),
        pltpu.make_async_copy(q_hbm.at[:, my_q], q_vm, load_sem.at[2]),
    ]
    for load in loads:
        load.start()

    barrier = pltpu.get_barrier_semaphore()
    pl.semaphore_signal(barrier, inc=1, device_id={"sub": other}, device_id_type=MESH)

    @pl.when(has_prev)
    def _():
        pl.semaphore_signal(barrier, inc=1, device_id={"seq": seq - 1}, device_id_type=MESH)

    @pl.when(has_next)
    def _():
        pl.semaphore_signal(barrier, inc=1, device_id={"seq": seq + 1}, device_id_type=MESH)

    peers = 1 + jnp.minimum(seq, 1) + jnp.minimum(n_seq - 1 - seq, 1)
    pl.semaphore_wait(barrier, peers)

    def remote(src, dst, send, recv, where):
        return pltpu.make_async_remote_copy(
            src_ref=src, dst_ref=dst, send_sem=send, recv_sem=recv, device_id=where, device_id_type=MESH
        )

    def piece_of(piece):
        return pl.ds(piece * piece_rows, piece_rows)

    swaps = [
        remote(
            hbm.at[piece_of(piece), its_cols], buf.at[0, sub, piece_of(piece)],
            swap_sem.at[piece, kind], recv_sem.at[0, sub, piece, kind], {"sub": other},
        )
        for piece in range(pieces)
        for kind, (hbm, buf) in enumerate(((k_hbm, kbuf), (v_hbm, vbuf)))
    ]
    for swap in swaps:
        swap.start()

    def hops(slot, part, piece):
        return [
            remote(
                buf.at[slot, part, piece_of(piece)], buf.at[slot + 1, part, piece_of(piece)],
                hop_sem.at[slot, part, piece, kind], recv_sem.at[slot + 1, part, piece, kind], {"seq": seq + 1},
            )
            for kind, buf in enumerate((kbuf, vbuf))
        ]

    def wait_arrival(slot, part, piece):
        for kind, buf in enumerate((kbuf, vbuf)):
            here = buf.at[slot, part, piece_of(piece)]
            pltpu.make_async_copy(here, here, recv_sem.at[slot, part, piece, kind]).wait()

    def start_hops(slot, part, piece):
        @pl.when(has_next)
        def _():
            for hop in hops(slot, part, piece):
                hop.start()

    loads[0].wait()
    loads[1].wait()
    for piece in range(pieces):
        start_hops(0, sub, piece)

    lane = lax.broadcasted_iota(jnp.int32, (1, LANES), 1)
    lows = jnp.full((1, LANES), 2**30, jnp.int32)
    highs = jnp.full((1, LANES), 2**30, jnp.int32)
    begin = jnp.int32(0)
    for d in range(n_docs):
        end = begin + lengths[d]
        lows = jnp.where(lane == d, begin, lows)
        highs = jnp.where(lane == d, end, highs)
        begin = end
    block = 256

    def fill(i, _):
        row0 = pl.multiple_of(i * block, block)
        base = lax.broadcasted_iota(jnp.int32, (block, LANES), 0) + row0 + seq * rows
        for slot in range(SPAN + 1):
            place = base - slot * rows
            inside = (place >= lows) & (place < highs)
            kx[slot, pl.ds(row0, block), :] = jnp.where(inside, 1.0, 0.0).astype(jnp.bfloat16)
            if slot == 0:
                qx[pl.ds(row0, block), :] = jnp.where(inside, 0.0, BLOCKED).astype(jnp.bfloat16)
        return 0

    lax.fori_loop(0, rows // block, fill, 0)

    for piece in range(pieces):
        wait_arrival(0, other, piece)
        start_hops(0, other, piece)
    loads[2].wait()

    def wide(x, times):
        return jnp.concatenate([x] * times, axis=1)

    def update(slot, part, key0, n_keys, row0, kv, first=False, offset=None, last=False):
        columns = pl.ds(pl.multiple_of(kv * DH, DH), DH)
        if part is None:
            spans = [(p, 0, min(half, n_keys - p * half)) for p in range(2) if n_keys > p * half]
        else:
            spans = [(part, key0, n_keys)]

        def rows_of(buf):
            return [buf[slot, p, pl.ds(k0, n), columns] for p, k0, n in spans]

        docs = [kx[slot, pl.ds(pl.multiple_of(p * half + k0, LANES), n), :] for p, k0, n in spans]
        keys = jnp.concatenate(
            [jnp.concatenate(rows_of(kbuf), axis=0), jnp.concatenate(docs, axis=0)], axis=1)
        vals = jnp.concatenate(
            [jnp.concatenate(rows_of(vbuf), axis=0), jnp.ones((n_keys, DH), jnp.bfloat16)], axis=1)
        q_rows = pl.ds(row0, rows_q)
        if offset is not None:
            row_at = lax.broadcasted_iota(jnp.int32, (rows_q, n_keys), 0) + offset
            causal = lax.broadcasted_iota(jnp.int32, (rows_q, n_keys), 1) <= row_at
        for g in range(group):
            h = kv * group + g
            at_h = pl.ds(pl.multiple_of(h * DH, DH), DH)
            query = jnp.concatenate([q_vm[q_rows, at_h], qx[q_rows, :]], axis=1)
            scores = lax.dot_general(
                query, keys, (((1,), (1,)), ((), ())), preferred_element_type=jnp.float32)
            if offset is not None:
                scores = jnp.where(causal, scores, LEAST)
            peak = jnp.max(scores, axis=1, keepdims=True)
            if first:
                new_top = jnp.broadcast_to(peak, (rows_q, LANES))
            else:
                old_top = top[h, q_rows, :]
                new_top = jnp.maximum(old_top, peak)
            weights = jnp.exp2((scores - wide(new_top, n_keys // LANES)) * SCALE).astype(jnp.bfloat16)
            total = jnp.dot(weights, vals, preferred_element_type=jnp.float32)
            if not first:
                factor = jnp.exp2((old_top - new_top) * SCALE)
                total = acc[h, q_rows, :] * wide(factor, 2) + total
            if last:
                obuf[q_rows, at_h] = (total[:, :DH] / total[:, DH:]).astype(jnp.bfloat16)
            else:
                acc[h, q_rows, :] = total
                top[h, q_rows, :] = new_top

    def sweep(slot, part, key0, n_keys, start, count, first=False, diagonal=False):
        def body(i, _):
            block_at, kv = i // kv_heads, i % kv_heads
            row0 = pl.multiple_of(start + block_at * rows_q, rows_q)
            update(slot, part, key0, n_keys, row0, kv, first, block_at * rows_q if diagonal else None)
            return 0

        lax.fori_loop(0, count * kv_heads, body, 0)

    blocks = rows // rows_q
    n_out = kv_heads * blocks

    def place(i):
        return i // blocks, pl.multiple_of((i % blocks) * rows_q, rows_q)

    def sends(i):
        kv, row0 = place(i)
        width = group * DH
        here = obuf.at[pl.ds(row0, rows_q), pl.ds(pl.multiple_of(kv * width, LANES), width)]
        there = out.at[pl.ds(row0, rows_q), pl.ds(pl.multiple_of(sub * q_cols + kv * width, LANES), width)]
        return (
            remote(here, there, out_send.at[i], out_recv.at[i], {"sub": other}),
            pltpu.make_async_copy(here, there, out_local.at[i]),
        )

    def finish(write):
        def body(i, _):
            write(*place(i))

            @pl.when(i > 0)
            def _():
                for copy in sends(i - 1):
                    copy.start()

            return 0

        lax.fori_loop(0, n_out, body, 0)
        sends(0)[1].wait()
        for copy in sends(n_out - 1):
            copy.start()

    for block_at in range(blocks):
        def own(kv, _):
            row0 = block_at * rows_q
            update(0, None, 0, row0 + rows_q, row0, kv, first=True, offset=row0)
            return 0

        lax.fori_loop(0, kv_heads, own, 0)

    for slot in range(1, SPAN + 1):
        @pl.when(seq >= slot)
        def _():
            for part in (sub, other):
                tail = slot == SPAN and part is other
                for piece in range(pieces):
                    wait_arrival(slot, part, piece)
                    if slot < SPAN:
                        start_hops(slot, part, piece)
                    if tail and piece < pieces - 1:
                        sweep(slot, part, piece * piece_rows, piece_rows, 0, blocks)
                if tail:
                    finish(lambda kv, row0: update(
                        slot, part, half - piece_rows, piece_rows, row0, kv, last=True))
                else:
                    sweep(slot, part, 0, half, 0, blocks)

    @pl.when(seq < SPAN)
    def _():
        def write(kv, row0):
            q_rows = pl.ds(row0, rows_q)
            for g in range(group):
                h = kv * group + g
                total = acc[h, q_rows, :]
                obuf[q_rows, pl.ds(pl.multiple_of(h * DH, DH), DH)] = (
                    total[:, :DH] / total[:, DH:]).astype(jnp.bfloat16)

        finish(write)

    for i in range(n_out):
        far, near = sends(i)
        far.wait()
        if i:
            near.wait()

    for swap in swaps:
        swap.wait_send()

    for slot in range(SPAN):
        @pl.when((seq >= slot) & has_next)
        def _():
            for part in (sub, other):
                for piece in range(pieces):
                    for hop in hops(slot, part, piece):
                        hop.wait_send()


def shards(n_seq, queries, keys, values, doc_lengths):
    rows, q_total = queries.shape
    half, kv_total = keys.shape
    q_cols = q_total // 2
    split_kv = kv_total // DH >= 2
    kv_cols = kv_total // 2 if split_kv else kv_total
    heads = q_cols // DH
    rows_q, pieces = min(512, half), 2
    sizes = (n_seq, rows, half, kv_cols, q_cols, split_kv, doc_lengths.shape[0], rows_q, pieces)
    n_out = kv_cols // DH * (rows // rows_q)
    any_space = pl.BlockSpec(memory_space=pl.ANY)
    dma = pltpu.SemaphoreType.DMA
    return pl.pallas_call(
        functools.partial(attention_kernel, sizes),
        out_shape=jax.ShapeDtypeStruct((rows, q_total), jnp.bfloat16),
        in_specs=[pl.BlockSpec(memory_space=pltpu.SMEM)] + [any_space] * 3,
        out_specs=any_space,
        scratch_shapes=[
            pltpu.VMEM((rows, q_cols), jnp.bfloat16),
            pltpu.VMEM((SPAN + 1, 2, half, kv_cols), jnp.bfloat16),
            pltpu.VMEM((SPAN + 1, 2, half, kv_cols), jnp.bfloat16),
            pltpu.VMEM((rows, LANES), jnp.bfloat16),
            pltpu.VMEM((SPAN + 1, rows, LANES), jnp.bfloat16),
            pltpu.VMEM((heads, rows, LANES), jnp.float32),
            pltpu.VMEM((heads, rows, 2 * DH), jnp.float32),
            pltpu.VMEM((rows, q_cols), jnp.bfloat16),
            dma((3,)),
            dma((pieces, 2)),
            dma((SPAN, 2, pieces, 2)),
            dma((SPAN + 1, 2, pieces, 2)),
            dma((n_out,)),
            dma((n_out,)),
            dma((n_out,)),
        ],
        compiler_params=pltpu.CompilerParams(
            collective_id=0, has_side_effects=True, vmem_limit_bytes=60 * 1024 * 1024
        ),
    )(doc_lengths, queries, keys, values)


def solution(mesh):
    placed = (
        P(("groups", "seq"), "head"),
        P(("groups", "seq", "sub"), "head"),
        P(("groups", "seq", "sub"), "head"),
        P("groups"),
    )
    return jax.shard_map(
        functools.partial(shards, mesh.shape["seq"]),
        mesh=mesh, in_specs=placed, out_specs=P(("groups", "seq"), "head"), check_vma=False,
    )
```
